128 devices in a mesh: gx: 16 (over y, x), gy: 8 (over z, core).
Axes of the slice: x: 4, y: 4, z: 4, core: 2. Of those that a mesh axis runs over, the one named last changes fastest.
Arguments:
- basis: float32 [32, 256, 128, 256], P(None, 'gx', 'gy'), may hold values from -0.09375 to 0.09375
- reaction: float32 [256, 128, 256], P('gx', 'gy'), may hold values from 0.5 to 4
Outputs:
- extended: float32 [32, 256, 128, 256], P(None, 'gx', 'gy')
- coarse: float32 [128, 5, 32, 32], replicated
The draws below stay inside these ranges and needn't reach their ends.
All inputs are finite; a program needn't handle non-finite values.
Results may differ from the reference program's by a relative error of at most 0.000071.
Values sent between devices are 32-bit elements; how exact they have to be, the bound alone decides.
A program may use at most 128 MiB of HBM per device.

```python
import math
import jax
import jax.numpy as jnp
from jax import lax

K = 32
SWEEPS = 4
CX = 16
CY = 16
CZ = 256
NX = 256
NY = 128
N_GX = 16
N_GY = 8


def level_of(rng, extent, shards, smallest, high):
    factor_of, own = 1.0, jax.random.fold_in(rng, 6)
    for axis_at, blocks in shards:
        draws = jnp.exp(jax.random.uniform(jax.random.fold_in(own, axis_at), (blocks,), jnp.float32, smallest / len(shards), high / len(shards)))
        factor_of = factor_of * jnp.repeat(draws, extent[axis_at] // blocks).reshape([-1 if axis == axis_at else 1 for axis in range(len(extent))])
    return factor_of


def centred(rng, extent, width, limit, shards=(), dtype=jnp.bfloat16):
    loudness = level_of(rng, extent, shards, -0.22, 0.18) if shards else 1.0
    result = jax.random.normal(rng, extent, jnp.float32) * width * loudness
    return jnp.minimum(jnp.maximum(result, -limit), limit).astype(dtype)


def setup_inputs(seed: int = 0) -> dict:
    keys = jax.random.split(jax.random.key(seed), 3)
    basis = centred(keys[0], (K, NX, NY, CZ), (CY * CZ) ** -0.5, 0.09375, ((1, 16), (2, 8)), jnp.float32)
    reaction = jnp.clip(jnp.exp(math.log(4.0) - 2.0794415 * jax.random.uniform(keys[1], (NX, NY, CZ), jnp.float32) ** level_of(keys[1], (NX, NY, CZ), ((0, 16), (1, 8)), -0.2, 0.2)), 0.5, 4.0)
    return dict(basis=basis, reaction=reaction)


OMEGA = 0.8


def stencil(field, coef):
    padded = jnp.pad(field, ((0, 0), (1, 1), (1, 1), (1, 1)))
    beside = padded[:, 2:, 1:-1, 1:-1] + padded[:, :-2, 1:-1, 1:-1]
    beside = beside + padded[:, 1:-1, 2:, 1:-1] + padded[:, 1:-1, :-2, 1:-1]
    beside = beside + padded[:, 1:-1, 1:-1, 2:] + padded[:, 1:-1, 1:-1, :-2]
    return (6.0 + coef) * field - beside


def extend_one(pair):
    phi, coef = pair
    kk, cx, cy, cz = phi.shape
    xpos = lax.broadcasted_iota(jnp.int32, (cx, cy, cz), 0)
    ypos = lax.broadcasted_iota(jnp.int32, (cx, cy, cz), 1)
    inner = (xpos >= 1) & (xpos <= cx - 2) & (ypos >= 1) & (ypos <= cy - 2)
    for sweep in range(SWEEPS):
        update = OMEGA * stencil(phi, coef) / (6.0 + coef)
        phi = phi - jnp.where(inner[None], update, jnp.float32(0.0))
    applied = stencil(phi, coef)
    diag = jnp.dot(phi.reshape(kk, -1), applied.reshape(kk, -1).T,
                   precision=lax.Precision.HIGHEST, preferred_element_type=jnp.float32)
    return phi, diag


def couple(own, other):
    return -jnp.einsum("iabyz,jabyz->abij", own, other, precision=lax.Precision.HIGHEST)


def reference(basis, reaction):
    gxn, gyn = N_GX, N_GY
    blocked = basis.reshape(K, gxn, CX, gyn, CY, CZ)
    subs = blocked.transpose(1, 3, 0, 2, 4, 5).reshape(gxn * gyn, K, CX, CY, CZ)
    coefs = reaction.reshape(gxn, CX, gyn, CY, CZ).transpose(0, 2, 1, 3, 4).reshape(gxn * gyn, CX, CY, CZ)
    phis, diags = lax.map(extend_one, (subs, coefs))
    extended = phis.reshape(gxn, gyn, K, CX, CY, CZ).transpose(2, 0, 3, 1, 4, 5).reshape(K, gxn * CX, gyn * CY, CZ)
    low_x = blocked[:, :, 0]
    high_x = blocked[:, :, CX - 1]
    zero_x = jnp.zeros_like(low_x[:, :1])
    minus_x = couple(low_x, jnp.concatenate([zero_x, high_x[:, :-1]], axis=1))
    plus_x = couple(high_x, jnp.concatenate([low_x[:, 1:], zero_x], axis=1))
    low_y = blocked[:, :, :, :, 0].transpose(0, 1, 3, 2, 4)
    high_y = blocked[:, :, :, :, CY - 1].transpose(0, 1, 3, 2, 4)
    zero_y = jnp.zeros_like(low_y[:, :, :1])
    minus_y = couple(low_y, jnp.concatenate([zero_y, high_y[:, :, :-1]], axis=2))
    plus_y = couple(high_y, jnp.concatenate([low_y[:, :, 1:], zero_y], axis=2))
    count = gxn * gyn
    coarse = jnp.stack([diags, minus_x.reshape(count, K, K), plus_x.reshape(count, K, K),
                        minus_y.reshape(count, K, K), plus_y.reshape(count, K, K)], axis=1)
    return extended, coarse
```

```python
import functools

import jax
import jax.numpy as jnp
from jax import lax
from jax.experimental import pallas as pl
from jax.experimental.pallas import tpu as pltpu
from jax.sharding import PartitionSpec as P

MESH = pl.DeviceIdType.MESH
ANY = pl.BlockSpec(memory_space=pl.ANY)
VM = pl.BlockSpec(memory_space=pltpu.VMEM)
OMEGA = 0.8
K, CX, CY, CZ = 32, 16, 16, 256
HALF = CZ // 2
HX = CY // 2
F32, BF16 = jnp.float32, jnp.bfloat16
LAG = 2
EDGES_AT, PARTS_AT, LINE_AT = 12, 14, 16


def split(v):
    hi = v.astype(BF16)
    return hi, (v - hi.astype(F32)).astype(BF16)


def lanes(rows):
    return lax.broadcasted_iota(jnp.int32, (rows, 128), 1)


def split_row(new, zin, slot, y):
    hi, lo = split(new)
    rows = pl.ds((y - 1) * K, K)
    zin[slot, rows, :CZ] = hi
    zin[slot, rows, CZ:] = lo


def sweep_row(src, dst, w, zin, zout, band, x):
    slot = lax.rem(x, 2)
    beside_z = jnp.dot(zin[slot], band[...], preferred_element_type=F32)
    low = src[x, 0]
    dst[x, 0] = low
    mid = src[x, 1]
    for y in range(1, CY - 1):
        high = src[x, y + 1]
        beside = (src[x - 1, y] + src[x + 1, y]) + (low + high)
        beside = beside + beside_z[(y - 1) * K:y * K]
        scaled = beside.reshape(K // 8, 8, CZ) * w[x, y][None]
        new = (1.0 - OMEGA) * mid + scaled.reshape(K, CZ)
        dst[x, y] = new
        if zout is not None:
            split_row(new, zout, slot, y)
        low, mid = mid, high
    dst[x, CY - 1] = mid


def product_row(phi, half, lhs, rhs, x, slot, bottom):
    last = lanes(K) == 127
    mid = phi[x, 0]
    for y in range(CY):
        d0, d1 = pltpu.roll(mid[:, :HALF], 127, 1), pltpu.roll(mid[:, HALF:], 127, 1)
        after = jnp.concatenate([jnp.where(last, d1, d0), jnp.where(last, 0.0, d1)], axis=1)
        out = (mid.reshape(K // 8, 8, CZ) * half[x, y][None]).reshape(K, CZ) - after
        high = None
        if y < CY - 1:
            high = phi[x, y + 1]
            out = out - high
        if not bottom:
            out = out - phi[x + 1, y]
        zs = pl.ds(y * CZ, CZ)
        hi, lo = split(mid)
        lhs[slot, :K, zs] = hi
        lhs[slot, K:, zs] = lo
        hi, lo = split(out)
        rhs[slot, :K, zs] = hi
        rhs[slot, K:, zs] = lo
        mid = high


def product(lhs, rhs):
    return lax.dot_general(lhs, rhs, (((1,), (1,)), ((), ())), preferred_element_type=F32)


def fold(total):
    return (total[:K, :K] + total[K:, K:]) + (total[:K, K:] + total[K:, :K])


def coefficients(reaction, w, half, x):
    for y in range(CY):
        d = 6.0 + reaction[x, pl.ds(y, 1), :]
        w[x, y] = jnp.broadcast_to(OMEGA / d, (8, CZ))
        half[x, y] = jnp.broadcast_to(0.5 * d, (8, CZ))


def pack(v, tall):
    tall[:, 0:K] = v
    out = tall[pl.ds(0, 8, stride=4), :]
    for r in range(1, 4):
        part = pltpu.roll(tall[pl.ds(r, 8, stride=4), :], 32 * r, 1)
        out = jnp.where(lanes(8) >= 32 * r, part, out)
    return out


def edge_product(own, other, count):
    total = jnp.zeros((2 * K, 2 * K), F32)
    for c in range(count):
        total = total + product(jnp.concatenate(split(own(c)), axis=0), jnp.concatenate(split(other(c)), axis=0))
    return -fold(total)


def main_kernel(n_gx, n_gy, basis, reaction, l4, rows, l0, l1, l2, l3, w, half, lhs, rhs, acc, band, z0, z1, z2, z3,
                got_xl, got_xu, got_yl, part, got_part, tall, edge, diag, ge, gd, wide,
                in_sem, face_send, face_recv, part_sem, e_send, e_recv, d_send, d_recv):
    gx, gy = lax.axis_index("gx"), lax.axis_index("gy")
    cx, cy, cz, core = gx % 4, gx // 4, gy // 2, gy % 2
    levels = (l0, l1, l2, l3, l4)
    zins = (z0, z1, z2, z3)
    twin = {"gx": gx, "gy": cz * 2 + (1 - core)}
    up_x, down_x, up_y = {"gx": gx + 1, "gy": gy}, {"gx": gx - 1, "gy": gy}, {"gx": gx, "gy": gy + 1}
    has_lx, has_ux, has_ly, has_uy = gx > 0, gx < n_gx - 1, gy > 0, gy < n_gy - 1
    beyond = {"gx": gx, "gy": lax.rem(gy + 2 * core + n_gy - 1, n_gy)}

    def on_line(n):
        return {"gx": gx, "gy": ((cz + n) % 4) * 2 + core}

    def on_plane(n):
        return {"gx": ((cy + n // 4) % 4) * 4 + (cx + n % 4) % 4, "gy": gy}

    barrier = pltpu.get_barrier_semaphore()

    def greet(device):
        pl.semaphore_signal(barrier, inc=1, device_id=device, device_id_type=MESH)

    for n in range(1, 4):
        greet(on_line(n))

    @pl.loop(1, 16)
    def _(n):
        greet(on_plane(n))

    greet(twin)
    greet(beyond)

    for x in (0, CX - 1, *range(1, CX - 1)):
        for y in range(CY):
            pltpu.make_async_copy(basis.at[:, x, y, :], l0.at[x, y], in_sem.at[x]).start()

    def arrived(x):
        pltpu.make_async_copy(l0.at[x], l0.at[x], in_sem.at[x]).wait()

    def seed(x):
        @pl.loop(0, CY)
        def _(y):
            v = l0[x, y]
            for level in range(1, 5):
                levels[level][x, y] = v

    def split_first(x):
        for y in range(1, CY - 1):
            split_row(l0[x, y], z0, lax.rem(x, 2), y)

    @pl.loop(0, CX)
    def _(x):
        coefficients(reaction, w, half, x)

    to = lax.broadcasted_iota(jnp.int32, (CZ, CZ), 1)
    at = lax.broadcasted_iota(jnp.int32, (CZ, CZ), 0)
    near = jnp.where(jnp.abs(to - at) == 1, 1.0, 0.0).astype(BF16)
    band[:CZ] = near
    band[CZ:] = near
    acc[...] = jnp.zeros_like(acc)
    edge[...] = jnp.zeros_like(edge)

    pl.semaphore_wait(barrier, 20)

    def face(src, dst, which, device):
        return pltpu.make_async_remote_copy(src, dst, face_send.at[which], face_recv.at[which], device_id=device, device_id_type=MESH)

    send_xl = face(l0.at[CX - 1, pl.ds(0, HX)], got_xl, 0, up_x)
    send_xu = face(l0.at[0, pl.ds(HX, HX)], got_xu, 1, down_x)
    send_y = face(l0.at[:, CY - 1], got_yl, 2, up_y)
    send_part = pltpu.make_async_remote_copy(part, got_part, part_sem.at[0], part_sem.at[1], device_id=up_x, device_id_type=MESH)

    arrived(0)
    arrived(CX - 1)

    @pl.when(has_ux)
    def _():
        send_xl.start()

    @pl.when(has_lx)
    def _():
        send_xu.start()

    seed(0)
    seed(CX - 1)
    arrived(1)
    split_first(1)

    def start_y_face():
        for x in range(4, CX - 1):
            arrived(x)

        @pl.when(has_uy)
        def _():
            send_y.start()

    def edges():
        @pl.when(has_ux)
        def _():
            send_xu.wait_recv()
            part[...] = pack(edge_product(lambda c: got_xu[c], lambda c: l0[CX - 1, HX + c], HX), tall)
            send_part.start()

        @pl.when(has_ly)
        def _():
            send_y.wait_recv()
            edge[8:16, :] = pack(edge_product(lambda c: l0[c, 0], lambda c: got_yl[c], CX), tall)

        @pl.when(has_lx)
        def _():
            send_xl.wait_recv()
            edge[0:8, :] = pack(edge_product(lambda c: l0[0, c], lambda c: got_xl[c], HX), tall)

    def remote(src, dst, sems, i, device):
        return pltpu.make_async_remote_copy(src, dst, sems[0].at[i], sems[1].at[i], device_id=device, device_id_type=MESH)

    def line_of(block, all_of, sems):
        height = block.shape[0]
        return lambda n: remote(block, all_of.at[gx, cz, pl.ds(core * height, height)], sems, 0, on_line(n))

    def plane_of(all_of, sems):
        height = all_of.shape[2] // 2
        mine = all_of.at[gx, :, pl.ds(core * height, height)]
        return lambda n: remote(mine, mine, sems, 1, on_plane(n))

    def twin_of(all_of, sems):
        height = all_of.shape[2] // 2
        mine = all_of.at[:, :, pl.ds(core * height, height)]
        return remote(mine, mine, sems, 2, twin)

    def line_start(block, all_of, sems):
        height = block.shape[0]
        for n in range(1, 4):
            line_of(block, all_of, sems)(n).start()
        all_of[gx, cz, pl.ds(pl.multiple_of(core * height, 8), height)] = block[...]

    def line_ref(all_of):
        return all_of.at[0, pl.ds(0, 3), pl.ds(0, all_of.shape[2] // 2)]

    def plane_ref(all_of):
        return all_of.at[pl.ds(0, 15), :, pl.ds(0, all_of.shape[2] // 2)]

    def all_recv(ref, sems, i):
        remote(ref, ref, sems, i, twin).wait_recv()

    def all_sent(ref, sems, i):
        remote(ref, ref, sems, i, twin).wait_send()

    def plane_start(all_of, sems):
        all_recv(line_ref(all_of), sems, 0)

        @pl.loop(1, 16)
        def _(n):
            plane_of(all_of, sems)(n).start()

    es, ds = (e_send, e_recv), (d_send, d_recv)

    def parts():
        @pl.when(has_lx)
        def _():
            send_part.wait_recv()
            edge[0:8, :] += got_part[...]

        line_start(edge, ge, es)

    def spread_edges():
        plane_start(ge, es)

    def step(t, active):
        if 7 in active:
            arrived(t + 1)
        if 6 in active:
            slot = lax.rem(t - 9, 2)
            acc[...] += product(lhs[slot], rhs[slot])
        if 5 in active:
            product_row(l4, half, lhs, rhs, t - 8, lax.rem(t - 8, 2), False)
        for s in (4, 3, 2, 1):
            if s in active:
                sweep_row(levels[s - 1], levels[s], w, zins[s - 1], zins[s] if s < 4 else None, band, t - LAG * (s - 1))
        if 0 in active:
            split_first(t + 1)

    def active_at(t):
        on = []
        if t <= 13:
            on.append(0)
        if t <= 2:
            on.append(7)
        for s in (1, 2, 3, 4):
            if 1 <= t - LAG * (s - 1) <= 14:
                on.append(s)
        if 0 <= t - 8 <= 14:
            on.append(5)
        if 0 <= t - 9 <= 14:
            on.append(6)
        return tuple(on)

    after = {2: start_y_face, EDGES_AT: edges, PARTS_AT: parts, LINE_AT: spread_edges}
    t = 1
    while t <= 23:
        end = t
        while end + 1 <= 23 and active_at(end + 1) == active_at(t) and end not in after:
            end += 1
        on = active_at(t)
        if end == t:
            step(jnp.int32(t), on)
        else:
            lax.fori_loop(t, end + 1, lambda i, c, on=on: (step(i, on), c)[1], 0)
        if end in after:
            after[end]()
        t = end + 1
    product_row(l4, half, lhs, rhs, CX - 1, 1, True)
    total = fold(acc[...] + product(lhs[1], rhs[1]))
    diag[...] = pack(total + total.T, tall)
    line_start(diag, gd, ds)

    all_recv(plane_ref(ge), es, 1)
    twin_of(ge, es).start()
    plane_start(gd, ds)
    twin_of(ge, es).wait_recv()

    flat = ge.reshape(n_gx * n_gy * 16, 128)
    for b, (lower, upper, shift) in enumerate(((1, 2, 128 - n_gy), (3, 4, 127))):
        for q in range(8):
            tile = flat[pl.ds(8 * b + q, 128, stride=16), :].T
            rows[pl.ds(lower * 1024 + q * 128, 128), :] = tile
            for r in range(4):
                wide[b, pl.ds((4 * q + r) * 40, 32), :] = tile[32 * r:32 * r + 32]

        @pl.loop(0, K)
        def _(i):
            for j in range(0, K, 8):
                got = wide[b, pl.ds(j * 40 + i, 8, stride=40), :]
                rows[pl.ds(pl.multiple_of(upper * 1024 + i * K, 8) + j, 8), :] = pltpu.roll(got, shift, 1)

    all_recv(plane_ref(gd), ds, 1)
    twin_of(gd, ds).start()
    twin_of(gd, ds).wait_recv()
    flat_d = gd.reshape(n_gx * n_gy * 8, 128)
    for q in range(8):
        rows[pl.ds(q * 128, 128), :] = flat_d[pl.ds(q, 128, stride=8), :].T

    @pl.when(has_ux)
    def _():
        send_xl.wait_send()
        send_part.wait_send()

    @pl.when(has_lx)
    def _():
        send_xu.wait_send()

    @pl.when(has_uy)
    def _():
        send_y.wait_send()

    for all_of, sems in ((ge, es), (gd, ds)):
        all_sent(line_ref(all_of), sems, 0)
        all_sent(plane_ref(all_of), sems, 1)
        twin_of(all_of, sems).wait_send()


def write_kernel(phi, rows, ext, out, sem, row_sem):
    for x in range(CX):
        for y in range(CY):
            pltpu.make_async_copy(phi.at[x, y], ext.at[:, x, y, :], sem).start()
    pltpu.make_async_copy(rows, out, row_sem).start()
    pltpu.make_async_copy(phi, phi, sem).wait()
    pltpu.make_async_copy(rows, out, row_sem).wait()


def everything(mesh, basis, reaction):
    n_gx, n_gy = mesh.shape["gx"], mesh.shape["gy"]
    n = n_gx * n_gy
    dma = pltpu.SemaphoreType.DMA
    level = pltpu.VMEM((CX, CY, K, CZ), F32)
    coef = pltpu.VMEM((CX, CY, 8, CZ), F32)
    operand = pltpu.VMEM((2, 2 * K, CY * CZ), BF16)
    halves = pltpu.VMEM((2, (CY - 2) * K, 2 * CZ), BF16)
    half_face, face = pltpu.VMEM((HX, K, CZ), F32), pltpu.VMEM((CX, K, CZ), F32)
    small = pltpu.VMEM((8, 128), F32)
    phi, rows = pl.pallas_call(
        functools.partial(main_kernel, n_gx, n_gy),
        out_shape=(pltpu.VMEM((CX, CY, K, CZ), F32), pltpu.VMEM((5 * K * K, n), F32)),
        in_specs=[ANY, VM],
        out_specs=(VM, VM),
        scratch_shapes=[
            level, level, level, level, coef, coef, operand, operand, pltpu.VMEM((2 * K, 2 * K), F32),
            pltpu.VMEM((2 * CZ, CZ), BF16), halves, halves, halves, halves,
            half_face, half_face, face, small, small, pltpu.VMEM((K, 128), F32), pltpu.VMEM((16, 128), F32), small,
            pltpu.VMEM((n_gx, n_gy // 2, 32, 128), F32), pltpu.VMEM((n_gx, n_gy // 2, 16, 128), F32),
            pltpu.VMEM((2, K * 40, 128), F32),
            dma((CX,)), dma((3,)), dma((3,)), dma((2,)), dma((3,)), dma((3,)), dma((3,)), dma((3,)),
        ],
        compiler_params=pltpu.CompilerParams(collective_id=0, has_side_effects=True, vmem_limit_bytes=50 * 1024 * 1024),
        name="everything",
    )(basis, reaction)
    return pl.pallas_call(
        write_kernel,
        out_shape=(jax.ShapeDtypeStruct(basis.shape, F32), jax.ShapeDtypeStruct(rows.shape, F32)),
        in_specs=[VM, VM],
        out_specs=(ANY, ANY),
        scratch_shapes=[dma, dma],
        compiler_params=pltpu.CompilerParams(vmem_limit_bytes=2 * 1024 * 1024),
        name="write",
    )(phi, rows)


def solution(mesh):
    def on_device(basis, reaction):
        extended, rows = everything(mesh, basis, reaction)
        coarse = rows.reshape(5, K, K, rows.shape[1]).transpose(3, 0, 1, 2)
        return extended, coarse

    return jax.shard_map(
        on_device,
        mesh=mesh,
        in_specs=(P(None, "gx", "gy", None), P("gx", "gy", None)),
        out_specs=(P(None, "gx", "gy", None), P()),
        check_vma=False,
    )
```

```python
import functools

import jax
import jax.numpy as jnp
from jax import lax
from jax.experimental import pallas as pl
from jax.experimental.pallas import tpu as pltpu
from jax.sharding import PartitionSpec as P

MESH = pl.DeviceIdType.MESH
ANY = pl.BlockSpec(memory_space=pl.ANY)
VM = pl.BlockSpec(memory_space=pltpu.VMEM)
OMEGA = 0.8
K, CX, CY, CZ = 32, 16, 16, 256
HALF = CZ // 2
HX = CY // 2
F32, BF16 = jnp.float32, jnp.bfloat16
LAG = 2
EDGES_AT, PARTS_AT, LINE_AT = 11, 12, 14


def split(v):
    hi = v.astype(BF16)
    return hi, (v - hi.astype(F32)).astype(BF16)


def lanes(rows):
    return lax.broadcasted_iota(jnp.int32, (rows, 128), 1)


def split_row(new, zin, slot, y):
    hi, lo = split(new)
    rows = pl.ds((y - 1) * K, K)
    zin[slot, rows, :CZ] = hi
    zin[slot, rows, CZ:] = lo


def sweep_row(src, dst, w, zin, zout, band, x):
    slot = lax.rem(x, 2)
    beside_z = jnp.dot(zin[slot], band[...], preferred_element_type=F32)
    low = src[x, 0]
    dst[x, 0] = low
    mid = src[x, 1]
    for y in range(1, CY - 1):
        high = src[x, y + 1]
        beside = (src[x - 1, y] + src[x + 1, y]) + (low + high)
        beside = beside + beside_z[(y - 1) * K:y * K]
        scaled = beside.reshape(K // 8, 8, CZ) * w[x, y][None]
        new = (1.0 - OMEGA) * mid + scaled.reshape(K, CZ)
        dst[x, y] = new
        if zout is not None:
            split_row(new, zout, slot, y)
        low, mid = mid, high
    dst[x, CY - 1] = mid


def product_row(phi, half, lhs, rhs, x, slot, bottom):
    last = lanes(K) == 127
    mid = phi[x, 0]
    for y in range(CY):
        d0, d1 = pltpu.roll(mid[:, :HALF], 127, 1), pltpu.roll(mid[:, HALF:], 127, 1)
        after = jnp.concatenate([jnp.where(last, d1, d0), jnp.where(last, 0.0, d1)], axis=1)
        out = (mid.reshape(K // 8, 8, CZ) * half[x, y][None]).reshape(K, CZ) - after
        high = None
        if y < CY - 1:
            high = phi[x, y + 1]
            out = out - high
        if not bottom:
            out = out - phi[x + 1, y]
        zs = pl.ds(y * CZ, CZ)
        hi, lo = split(mid)
        lhs[slot, :K, zs] = hi
        lhs[slot, K:, zs] = lo
        hi, lo = split(out)
        rhs[slot, :K, zs] = hi
        rhs[slot, K:, zs] = lo
        mid = high


def product(lhs, rhs):
    return lax.dot_general(lhs, rhs, (((1,), (1,)), ((), ())), preferred_element_type=F32)


def fold(total):
    return (total[:K, :K] + total[K:, K:]) + (total[:K, K:] + total[K:, :K])


def coefficients(reaction, w, half, x):
    for y in range(CY):
        d = 6.0 + reaction[x, pl.ds(y, 1), :]
        w[x, y] = jnp.broadcast_to(OMEGA / d, (8, CZ))
        half[x, y] = jnp.broadcast_to(0.5 * d, (8, CZ))


def pack(v, tall):
    tall[:, 0:K] = v
    out = tall[pl.ds(0, 8, stride=4), :]
    for r in range(1, 4):
        part = pltpu.roll(tall[pl.ds(r, 8, stride=4), :], 32 * r, 1)
        out = jnp.where(lanes(8) >= 32 * r, part, out)
    return out


def edge_product(own, other, count):
    total = jnp.zeros((2 * K, 2 * K), F32)
    for c in range(count):
        total = total + product(jnp.concatenate(split(own(c)), axis=0), jnp.concatenate(split(other(c)), axis=0))
    return -fold(total)


def main_kernel(n_gx, n_gy, basis, reaction, l4, rows, l0, l1, l2, l3, w, half, lhs, rhs, acc, band, z0, z1, z2, z3,
                got_xl, got_xu, got_yl, part, got_part, tall, edge, diag, ge, gd, wide,
                in_sem, face_send, face_recv, part_sem, e_send, e_recv, d_send, d_recv):
    gx, gy = lax.axis_index("gx"), lax.axis_index("gy")
    cx, cy, cz, core = gx % 4, gx // 4, gy // 2, gy % 2
    levels = (l0, l1, l2, l3, l4)
    zins = (z0, z1, z2, z3)
    twin = {"gx": gx, "gy": cz * 2 + (1 - core)}
    up_x, down_x, up_y = {"gx": gx + 1, "gy": gy}, {"gx": gx - 1, "gy": gy}, {"gx": gx, "gy": gy + 1}
    has_lx, has_ux, has_ly, has_uy = gx > 0, gx < n_gx - 1, gy > 0, gy < n_gy - 1
    beyond = {"gx": gx, "gy": lax.rem(gy + 2 * core + n_gy - 1, n_gy)}

    def on_line(n):
        return {"gx": gx, "gy": ((cz + n) % 4) * 2 + core}

    def on_plane(n):
        return {"gx": ((cy + n // 4) % 4) * 4 + (cx + n % 4) % 4, "gy": gy}

    barrier = pltpu.get_barrier_semaphore()

    def greet(device):
        pl.semaphore_signal(barrier, inc=1, device_id=device, device_id_type=MESH)

    for n in range(1, 4):
        greet(on_line(n))

    @pl.loop(1, 16)
    def _(n):
        greet(on_plane(n))

    greet(twin)
    greet(beyond)

    @pl.loop(0, CX)
    def _(i):
        x = jnp.where(i == 1, CX - 1, jnp.where(i == 0, 0, i - 1))
        for y in range(CY):
            pltpu.make_async_copy(basis.at[:, x, y, :], l0.at[x, y], in_sem.at[x]).start()
        coefficients(reaction, w, half, x)

    def arrived(x):
        pltpu.make_async_copy(l0.at[x], l0.at[x], in_sem.at[x]).wait()

    def seed(x):
        @pl.loop(0, CY)
        def _(y):
            v = l0[x, y]
            for level in range(1, 5):
                levels[level][x, y] = v

    def split_first(x):
        for y in range(1, CY - 1):
            split_row(l0[x, y], z0, lax.rem(x, 2), y)

    to = lax.broadcasted_iota(jnp.int32, (CZ, CZ), 1)
    at = lax.broadcasted_iota(jnp.int32, (CZ, CZ), 0)
    near = jnp.where(jnp.abs(to - at) == 1, 1.0, 0.0).astype(BF16)
    band[:CZ] = near
    band[CZ:] = near
    acc[...] = jnp.zeros_like(acc)
    edge[...] = jnp.zeros_like(edge)

    pl.semaphore_wait(barrier, 20)

    def face(src, dst, which, device):
        return pltpu.make_async_remote_copy(src, dst, face_send.at[which], face_recv.at[which], device_id=device, device_id_type=MESH)

    send_xl = face(l0.at[CX - 1, pl.ds(0, HX)], got_xl, 0, up_x)
    send_xu = face(l0.at[0, pl.ds(HX, HX)], got_xu, 1, down_x)
    send_y = face(l0.at[:, CY - 1], got_yl, 2, up_y)
    send_part = pltpu.make_async_remote_copy(part, got_part, part_sem.at[0], part_sem.at[1], device_id=up_x, device_id_type=MESH)

    arrived(0)
    arrived(CX - 1)

    @pl.when(has_ux)
    def _():
        send_xl.start()

    @pl.when(has_lx)
    def _():
        send_xu.start()

    seed(0)
    seed(CX - 1)
    arrived(1)
    split_first(1)

    def start_y_face():
        for x in range(4, CX - 1):
            arrived(x)

        @pl.when(has_uy)
        def _():
            send_y.start()

    def edges():
        @pl.when(has_ux)
        def _():
            send_xu.wait_recv()
            part[...] = pack(edge_product(lambda c: got_xu[c], lambda c: l0[CX - 1, HX + c], HX), tall)
            send_part.start()

        @pl.when(has_ly)
        def _():
            send_y.wait_recv()
            edge[8:16, :] = pack(edge_product(lambda c: l0[c, 0], lambda c: got_yl[c], CX), tall)

        @pl.when(has_lx)
        def _():
            send_xl.wait_recv()
            edge[0:8, :] = pack(edge_product(lambda c: l0[0, c], lambda c: got_xl[c], HX), tall)

    def remote(src, dst, sems, i, device):
        return pltpu.make_async_remote_copy(src, dst, sems[0].at[i], sems[1].at[i], device_id=device, device_id_type=MESH)

    def line_of(block, all_of, sems):
        height = block.shape[0]
        return lambda n: remote(block, all_of.at[gx, cz, pl.ds(core * height, height)], sems, 0, on_line(n))

    def plane_of(all_of, sems):
        height = all_of.shape[2] // 2
        mine = all_of.at[gx, :, pl.ds(core * height, height)]
        return lambda n: remote(mine, mine, sems, 1, on_plane(n))

    def twin_of(all_of, sems):
        height = all_of.shape[2] // 2
        mine = all_of.at[:, :, pl.ds(core * height, height)]
        return remote(mine, mine, sems, 2, twin)

    def line_start(block, all_of, sems):
        height = block.shape[0]
        for n in range(1, 4):
            line_of(block, all_of, sems)(n).start()
        all_of[gx, cz, pl.ds(pl.multiple_of(core * height, 8), height)] = block[...]

    def line_ref(all_of):
        return all_of.at[0, pl.ds(0, 3), pl.ds(0, all_of.shape[2] // 2)]

    def plane_ref(all_of):
        return all_of.at[pl.ds(0, 15), :, pl.ds(0, all_of.shape[2] // 2)]

    def all_recv(ref, sems, i):
        remote(ref, ref, sems, i, twin).wait_recv()

    def all_sent(ref, sems, i):
        remote(ref, ref, sems, i, twin).wait_send()

    def plane_start(all_of, sems):
        all_recv(line_ref(all_of), sems, 0)

        @pl.loop(1, 16)
        def _(n):
            plane_of(all_of, sems)(n).start()

    es, ds = (e_send, e_recv), (d_send, d_recv)

    def parts():
        @pl.when(has_lx)
        def _():
            send_part.wait_recv()
            edge[0:8, :] += got_part[...]

        line_start(edge, ge, es)

    def spread_edges():
        plane_start(ge, es)

    def step(t, carry):
        @pl.when(t <= 2)
        def _():
            arrived(t + 1)

        @pl.when(t >= 9)
        def _():
            slot = lax.rem(t - 9, 2)
            acc[...] += product(lhs[slot], rhs[slot])

        @pl.when(jnp.logical_and(t >= 8, t <= 22))
        def _():
            product_row(l4, half, lhs, rhs, t - 8, lax.rem(t - 8, 2), False)

        for s in (4, 3, 2, 1):
            x = t - LAG * (s - 1)

            @pl.when(jnp.logical_and(x >= 1, x <= CX - 2))
            def _(s=s, x=x):
                sweep_row(levels[s - 1], levels[s], w, zins[s - 1], zins[s] if s < 4 else None, band, x)

        @pl.when(t <= 13)
        def _():
            split_first(t + 1)

        for when, event in ((2, start_y_face), (EDGES_AT, edges), (PARTS_AT, parts), (LINE_AT, spread_edges)):
            pl.when(t == when)(event)
        return carry

    lax.fori_loop(1, 24, step, 0)
    product_row(l4, half, lhs, rhs, CX - 1, 1, True)
    total = fold(acc[...] + product(lhs[1], rhs[1]))
    diag[...] = pack(total + total.T, tall)
    line_start(diag, gd, ds)

    all_recv(plane_ref(ge), es, 1)
    twin_of(ge, es).start()
    plane_start(gd, ds)
    twin_of(ge, es).wait_recv()

    flat = ge.reshape(n_gx * n_gy * 16, 128)
    for b, (lower, upper, shift) in enumerate(((1, 2, 128 - n_gy), (3, 4, 127))):
        for q in range(8):
            tile = flat[pl.ds(8 * b + q, 128, stride=16), :].T
            rows[pl.ds(lower * 1024 + q * 128, 128), :] = tile
            for r in range(4):
                wide[b, pl.ds((4 * q + r) * 40, 32), :] = tile[32 * r:32 * r + 32]

        @pl.loop(0, K)
        def _(i):
            for j in range(0, K, 8):
                got = wide[b, pl.ds(j * 40 + i, 8, stride=40), :]
                rows[pl.ds(pl.multiple_of(upper * 1024 + i * K, 8) + j, 8), :] = pltpu.roll(got, shift, 1)

    all_recv(plane_ref(gd), ds, 1)
    twin_of(gd, ds).start()
    twin_of(gd, ds).wait_recv()
    flat_d = gd.reshape(n_gx * n_gy * 8, 128)
    for q in range(8):
        rows[pl.ds(q * 128, 128), :] = flat_d[pl.ds(q, 128, stride=8), :].T

    @pl.when(has_ux)
    def _():
        send_xl.wait_send()
        send_part.wait_send()

    @pl.when(has_lx)
    def _():
        send_xu.wait_send()

    @pl.when(has_uy)
    def _():
        send_y.wait_send()

    for all_of, sems in ((ge, es), (gd, ds)):
        all_sent(line_ref(all_of), sems, 0)
        all_sent(plane_ref(all_of), sems, 1)
        twin_of(all_of, sems).wait_send()


def write_kernel(phi, rows, ext, out, sem, row_sem):
    pltpu.make_async_copy(rows, out, row_sem).start()

    @pl.loop(0, CX)
    def _(x):
        for y in range(CY):
            pltpu.make_async_copy(phi.at[x, y], ext.at[:, x, y, :], sem).start()

    pltpu.make_async_copy(phi, phi, sem).wait()
    pltpu.make_async_copy(rows, out, row_sem).wait()


def everything(mesh, basis, reaction):
    n_gx, n_gy = mesh.shape["gx"], mesh.shape["gy"]
    n = n_gx * n_gy
    dma = pltpu.SemaphoreType.DMA
    level = pltpu.VMEM((CX, CY, K, CZ), F32)
    coef = pltpu.VMEM((CX, CY, 8, CZ), F32)
    operand = pltpu.VMEM((2, 2 * K, CY * CZ), BF16)
    halves = pltpu.VMEM((2, (CY - 2) * K, 2 * CZ), BF16)
    half_face, face = pltpu.VMEM((HX, K, CZ), F32), pltpu.VMEM((CX, K, CZ), F32)
    small = pltpu.VMEM((8, 128), F32)
    phi, rows = pl.pallas_call(
        functools.partial(main_kernel, n_gx, n_gy),
        out_shape=(pltpu.VMEM((CX, CY, K, CZ), F32), pltpu.VMEM((5 * K * K, n), F32)),
        in_specs=[ANY, VM],
        out_specs=(VM, VM),
        scratch_shapes=[
            level, level, level, level, coef, coef, operand, operand, pltpu.VMEM((2 * K, 2 * K), F32),
            pltpu.VMEM((2 * CZ, CZ), BF16), halves, halves, halves, halves,
            half_face, half_face, face, small, small, pltpu.VMEM((K, 128), F32), pltpu.VMEM((16, 128), F32), small,
            pltpu.VMEM((n_gx, n_gy // 2, 32, 128), F32), pltpu.VMEM((n_gx, n_gy // 2, 16, 128), F32),
            pltpu.VMEM((2, K * 40, 128), F32),
            dma((CX,)), dma((3,)), dma((3,)), dma((2,)), dma((3,)), dma((3,)), dma((3,)), dma((3,)),
        ],
        compiler_params=pltpu.CompilerParams(collective_id=0, has_side_effects=True, vmem_limit_bytes=50 * 1024 * 1024),
        name="everything",
    )(basis, reaction)
    return pl.pallas_call(
        write_kernel,
        out_shape=(jax.ShapeDtypeStruct(basis.shape, F32), jax.ShapeDtypeStruct(rows.shape, F32)),
        in_specs=[VM, VM],
        out_specs=(ANY, ANY),
        scratch_shapes=[dma, dma],
        compiler_params=pltpu.CompilerParams(vmem_limit_bytes=2 * 1024 * 1024),
        name="write",
    )(phi, rows)


def solution(mesh):
    def on_device(basis, reaction):
        extended, rows = everything(mesh, basis, reaction)
        coarse = rows.reshape(5, K, K, rows.shape[1]).transpose(3, 0, 1, 2)
        return extended, coarse

    return jax.shard_map(
        on_device,
        mesh=mesh,
        in_specs=(P(None, "gx", "gy", None), P("gx", "gy", None)),
        out_specs=(P(None, "gx", "gy", None), P()),
        check_vma=False,
    )
```
